32 devices in a mesh: row: 8 (over z, x), col: 4 (over y, core).
Axes of the slice: x: 2, y: 2, z: 4, core: 2. Of those that a mesh axis runs over, the one named last changes fastest.
Arguments:
- eigvecs: bfloat16 [49152, 4096], P('row', 'col'), may hold values from -41 to 41
- reflectors: bfloat16 [8, 49152, 128], P(None, 'row'), as said below
- factors: float32 [8, 128, 128], replicated, as said below
Outputs:
- vectors: bfloat16 [49152, 4096], P('row', 'col')
- deviation: float32 [4096], P('col')
The draws below stay inside these ranges and needn't reach their ends.
Inputs may be any that keep to these rules, and one draw needn't show every extreme that they name: `reflectors`: each panel's vectors are dense and linearly independent. factors[k] is the upper triangular compact WY factor of reflectors[k]: its inverse plus its inverse's transpose equals reflectors[k]^T reflectors[k], so that I - reflectors[k] factors[k] reflectors[k]^T is orthogonal up to rounding.
All inputs are finite; a program needn't handle non-finite values.
Results may differ from the reference program's by a relative error of at most 0.014.
Values may be sent and summed in bfloat16 or wider, within the bound.
A program may use at most 128 MiB of HBM per device.

```python
import jax
import jax.numpy as jnp
from jax import lax

NORD = 49152
M = 4096
B = 128
PANELS = 8


def reflector_panels(key):
    base = jax.random.fold_in(key, 7)
    first = jax.random.fold_in(base, 1)
    second = jax.random.fold_in(base, 2)
    third = jax.random.fold_in(base, 3)
    rough = jnp.clip(jax.random.normal(first, (PANELS, NORD, B), jnp.float32), -6.0, 6.0)
    weight = 0.4
    shared = jnp.clip(jax.random.normal(second, (PANELS, NORD, 1), jnp.float32), -6.0, 6.0)
    mixing = weight * jnp.clip(jax.random.normal(third, (PANELS, 1, B), jnp.float32), -6.0, 6.0)
    panels = (rough + shared * mixing) * NORD ** (-0.5)
    return panels.astype(jnp.bfloat16)


def draw_reflectors(key, part):
    return reflector_panels(key)


def draw_factors(key, part):
    panels = reflector_panels(key).astype(jnp.float32)
    gram = jnp.einsum('knb,knc->kbc', panels, panels, precision=lax.Precision.HIGHEST)
    eye = jnp.eye(B, dtype=jnp.float32)
    inverse = jnp.triu(gram, 1) + 0.5 * gram * eye[None, :, :]

    def invert(upper):
        return jax.scipy.linalg.solve_triangular(upper, eye, lower=False)
    return jax.vmap(invert)(inverse).astype(jnp.float32)


def draw_eigvecs(key, part):
    first = jax.random.fold_in(key, 21)
    second = jax.random.fold_in(key, 22)
    third = jax.random.fold_in(key, 23)
    fourth = jax.random.fold_in(key, 24)
    rows = jnp.arange(NORD).astype(jnp.float32) / NORD
    phase = jax.random.uniform(fourth, (), jnp.float32, 0.0, 1.0)
    entries = jnp.clip(jax.random.normal(first, (NORD, M), jnp.float32), -6.0, 6.0)
    amplitude = 0.8
    smooth = jnp.exp(amplitude * jnp.sin(6.2831853 * (2.0 * rows + phase)))
    rough = jnp.exp(jax.random.uniform(second, (NORD,), jnp.float32, -0.6931472, 0.6931472))
    columns = jnp.exp(jax.random.uniform(third, (M,), jnp.float32, -0.6931472, 0.4054651))
    values = entries * (smooth * rough)[:, None] * columns[None, :]
    return values.astype(jnp.bfloat16)


def setup_inputs(seed: int = 0) -> dict:
    seeds = jax.random.split(jax.random.key(seed), 4)
    return {
        "eigvecs": draw_eigvecs(jax.random.fold_in(seeds[3], 71), 0),
        "reflectors": draw_reflectors(jax.random.fold_in(seeds[3], 71), 0),
        "factors": draw_factors(jax.random.fold_in(seeds[3], 71), 0),
    }


def reference(eigvecs, reflectors, factors):
    vectors = eigvecs
    for panel in range(PANELS):
        basis = reflectors[panel]
        proj = jnp.dot(basis.T.astype(jnp.float32), vectors.astype(jnp.float32), preferred_element_type=jnp.float32)
        scaled = jnp.dot(factors[panel], proj, precision=lax.Precision.HIGHEST).astype(jnp.bfloat16)
        update = jnp.dot(basis.astype(jnp.float32), scaled.astype(jnp.float32), preferred_element_type=jnp.float32)
        vectors = (vectors.astype(jnp.float32) - update).astype(jnp.bfloat16)
    wide = vectors.astype(jnp.float32)
    squares = lax.optimization_barrier(jnp.sum(wide * wide, axis=0))
    deviation = jnp.sqrt(squares / NORD) - 1.0
    return (vectors, deviation)
```

```python
import functools
import math

import jax
import jax.numpy as jnp
from jax import lax
from jax.experimental import pallas as pl
from jax.experimental.pallas import tpu as pltpu
from jax.sharding import PartitionSpec as P

MESH = pl.DeviceIdType.MESH
TN = (((0,), (0,)), ((), ()))
NT = (((1,), (1,)), ((), ()))


def settle(ref, sem):
    pltpu.make_async_copy(ref, ref, sem).wait()


def send(src, dst, sent, got, where):
    pltpu.make_async_remote_copy(
        src_ref=src, dst_ref=dst, send_sem=sent, recv_sem=got, device_id=where, device_id_type=MESH
    ).start()


def greet(axes):
    barrier = pltpu.get_barrier_semaphore()
    for axis, size in axes:
        me = lax.axis_index(axis)

        def hello(d, carry, axis=axis, size=size, me=me):
            pl.semaphore_signal(
                barrier, inc=1, device_id={axis: lax.rem(me + d, size)}, device_id_type=MESH
            )
            return carry

        lax.fori_loop(1, size, hello, 0)
    pl.semaphore_wait(barrier, sum(size - 1 for _, size in axes))


def scale_kernel(
    rows, cols, chunks,
    e_hbm, r_hbm, f_ref, out_hbm,
    ebuf, rbuf, acc, psend, precv, gsend, grecv, gbuf, xbuf, sbuf,
    e_sem, r_sem, p_sent, p_got, g_sent, g_got, h_sent, h_got, c_sent, c_got, s_sent, s_got, o_sem,
):
    panels, local, width = r_hbm.shape
    total = panels * width
    cw = ebuf.shape[2] // rows
    span = ebuf.shape[2]
    gs = gsend.shape[0] // rows
    depth = math.gcd(local, 1024)
    steps = local // depth
    row, col = lax.axis_index("row"), lax.axis_index("col")

    def load_r(k):
        return pltpu.make_async_copy(
            r_hbm.at[k], rbuf.at[:, pl.ds(k * width, width)], r_sem.at[k]
        )

    def load_e(j):
        return pltpu.make_async_copy(
            e_hbm.at[:, pl.ds(j * span, span)], ebuf.at[j], e_sem.at[j]
        )

    for k in range(panels):
        load_r(k).start()
    for j in range(chunks):
        load_e(j).start()
    greet((("row", rows), ("col", cols)))
    for k in range(panels):
        load_r(k).wait()

    high = panels - 1 - col

    def block(t, carry):
        flag = t // high
        panel = high + flag * (col - high)
        prior = t - flag * high

        def step(i, total_block):
            at = pl.ds(pl.multiple_of(i * depth, depth), depth)
            a = rbuf[at, pl.ds(pl.multiple_of(prior * width, width), width)]
            b = rbuf[at, pl.ds(pl.multiple_of(panel * width, width), width)]
            return total_block + lax.dot_general(a, b, TN, preferred_element_type=jnp.float32)

        result = lax.fori_loop(0, steps, step, jnp.zeros((width, width), jnp.float32))
        gsend[pl.ds(pl.multiple_of(t * width, width), width), :] = result.astype(jnp.bfloat16)
        return carry

    lax.fori_loop(0, panels, block, 0)

    def send_gram(d, carry):
        peer = lax.rem(row + d, rows)
        send(
            gsend.at[pl.ds(pl.multiple_of(peer * gs, gs), gs), :], grecv.at[d - 1],
            g_sent, g_got, {"row": peer},
        )
        return carry

    lax.fori_loop(1, rows, send_gram, 0)

    mine = pl.ds(pl.multiple_of(row * gs, gs), gs)

    def share_gram_rows():
        settle(grecv, g_got)
        part = gsend[mine, :].astype(jnp.float32)
        for d in range(rows - 1):
            part = part + grecv[d].astype(jnp.float32)
        gbuf[col, mine, :] = part.astype(jnp.bfloat16)

        def go(d, carry):
            peer = lax.rem(row + d, rows)
            send(gbuf.at[col, mine, :], gbuf.at[col, mine, :], h_sent, h_got, {"row": peer})
            return carry

        lax.fori_loop(1, rows, go, 0)

    def share_gram_cols():
        settle(gbuf.at[col, pl.ds(0, (rows - 1) * gs), :], h_got)

        def go(d, carry):
            peer = lax.rem(col + d, cols)
            send(gbuf.at[col], gbuf.at[col], c_sent, c_got, {"col": peer})
            return carry

        lax.fori_loop(1, cols, go, 0)

    for j in range(chunks):
        load_e(j).wait()
        acc[...] = jnp.zeros_like(acc)

        def step(i, carry, j=j):
            at = pl.ds(pl.multiple_of(i * depth, depth), depth)
            acc[...] += lax.dot_general(
                ebuf[j, at, :], rbuf[at, :], TN, preferred_element_type=jnp.float32
            )
            return carry

        lax.fori_loop(0, steps, step, 0)
        psend[j] = acc[...].astype(jnp.bfloat16)

        def send_proj(d, carry, j=j):
            peer = lax.rem(row + d, rows)
            send(
                psend.at[j, pl.ds(pl.multiple_of(peer * cw, cw), cw), :], precv.at[j, d - 1],
                p_sent.at[j], p_got.at[j], {"row": peer},
            )
            return carry

        lax.fori_loop(1, rows, send_proj, 0)
        if j == 0:
            share_gram_rows()
        if j == min(1, chunks - 1):
            share_gram_cols()

    own = pl.ds(pl.multiple_of(row * cw, cw), cw)
    for j in range(chunks):
        settle(precv.at[j], p_got.at[j])
        part = psend[j, own, :].astype(jnp.float32)
        for d in range(rows - 1):
            part = part + precv[j, d].astype(jnp.float32)
        xbuf[pl.ds(j * cw, cw), :] = part
    settle(gbuf.at[pl.ds(0, cols - 1)], c_got)

    done = []
    for k in range(panels):
        part = xbuf[:, k * width : (k + 1) * width]
        if k:
            place = min(k, panels - 1 - k)
            start = 0 if k >= cols else (panels - 1 - k) * width
            cross = gbuf[place, start : start + k * width, :]
            part = part - jnp.dot(
                jnp.concatenate(done, axis=1), cross, preferred_element_type=jnp.float32
            )
        part = lax.dot_general(
            part, f_ref[k], NT,
            precision=lax.Precision.HIGHEST, preferred_element_type=jnp.float32,
        ).astype(jnp.bfloat16)
        done.append(part)
        for j in range(chunks):
            sbuf[j, own, k * width : (k + 1) * width] = part[j * cw : (j + 1) * cw]

    def send_scaled(d, carry):
        peer = lax.rem(row + d, rows)
        send(sbuf.at[:, own, :], sbuf.at[:, own, :], s_sent, s_got, {"row": peer})
        return carry

    lax.fori_loop(1, rows, send_scaled, 0)
    settle(grecv, g_sent)
    settle(gbuf.at[col, pl.ds(0, (rows - 1) * gs), :], h_sent)
    settle(gbuf.at[pl.ds(0, cols - 1)], c_sent)
    for j in range(chunks):
        settle(precv.at[j], p_sent.at[j])
    rest = sbuf.at[:, pl.ds(0, (rows - 1) * cw), :]
    settle(rest, s_got)
    settle(rest, s_sent)
    result = pltpu.make_async_copy(sbuf, out_hbm, o_sem)
    result.start()
    result.wait()


def find_scaled(eigvecs, reflectors, factors, rows, cols):
    local, columns = eigvecs.shape
    panels, _, width = reflectors.shape
    total = panels * width
    chunks = max(1, min(4, columns // rows // 16, columns // 128))
    span = columns // chunks
    cw = span // rows
    gs = total // rows
    any_spec = pl.BlockSpec(memory_space=pl.ANY)
    dma = pltpu.SemaphoreType.DMA
    low = jnp.bfloat16
    scaled = pl.pallas_call(
        functools.partial(scale_kernel, rows, cols, chunks),
        out_shape=jax.ShapeDtypeStruct((chunks, span, total), low),
        in_specs=[any_spec, any_spec, pl.BlockSpec(memory_space=pltpu.VMEM)],
        out_specs=any_spec,
        scratch_shapes=[
            pltpu.VMEM((chunks, local, span), low),
            pltpu.VMEM((local, total), low),
            pltpu.VMEM((span, total), jnp.float32),
            pltpu.VMEM((chunks, span, total), low),
            pltpu.VMEM((chunks, rows - 1, cw, total), low),
            pltpu.VMEM((total, width), low),
            pltpu.VMEM((rows - 1, gs, width), low),
            pltpu.VMEM((cols, total, width), low),
            pltpu.VMEM((chunks * cw, total), jnp.float32),
            pltpu.VMEM((chunks, span, total), low),
            dma((chunks,)), dma((panels,)), dma((chunks,)), dma((chunks,)),
            dma, dma, dma, dma, dma, dma, dma, dma, dma,
        ],
        compiler_params=pltpu.CompilerParams(
            collective_id=0, has_side_effects=True, vmem_limit_bytes=60 * 1024 * 1024
        ),
    )(eigvecs, reflectors, factors)
    return scaled.reshape(columns, total)


def update_kernel(e_ref, r_ref, s_ref, v_ref, q_ref):
    panels = r_ref.shape[0]
    stacked = jnp.concatenate([r_ref[k] for k in range(panels)], axis=1)
    update = lax.dot_general(stacked, s_ref[...], NT, preferred_element_type=jnp.float32)
    vectors = (e_ref[...].astype(jnp.float32) - update).astype(jnp.bfloat16)
    v_ref[...] = vectors
    wide = vectors.astype(jnp.float32)
    squares = jnp.sum((wide * wide).reshape(-1, 8, wide.shape[1]), axis=0)

    @pl.when(pl.program_id(0) == 0)
    def _():
        q_ref[...] = jnp.zeros_like(q_ref)

    q_ref[...] += squares


def update_vectors(eigvecs, reflectors, scaled):
    local, columns = eigvecs.shape
    panels, _, width = reflectors.shape
    tile = math.gcd(local, 512)
    return pl.pallas_call(
        update_kernel,
        grid=(local // tile,),
        out_shape=(
            jax.ShapeDtypeStruct((local, columns), jnp.bfloat16),
            jax.ShapeDtypeStruct((8, columns), jnp.float32),
        ),
        in_specs=[
            pl.BlockSpec((tile, columns), lambda i: (i, 0)),
            pl.BlockSpec((panels, tile, width), lambda i: (0, i, 0)),
            pl.BlockSpec((columns, panels * width), lambda i: (0, 0)),
        ],
        out_specs=(
            pl.BlockSpec((tile, columns), lambda i: (i, 0)),
            pl.BlockSpec((8, columns), lambda i: (0, 0)),
        ),
        compiler_params=pltpu.CompilerParams(
            dimension_semantics=("arbitrary",), vmem_limit_bytes=60 * 1024 * 1024
        ),
    )(eigvecs, reflectors, scaled)


def norm_kernel(rows, q_ref, out_ref, got, sent_sem, got_sem):
    row = lax.axis_index("row")
    greet((("row", rows),))

    def go(d, carry):
        send(q_ref, got.at[d - 1], sent_sem, got_sem, {"row": lax.rem(row + d, rows)})
        return carry

    lax.fori_loop(1, rows, go, 0)
    settle(got, got_sem)
    part = q_ref[...]
    for d in range(rows - 1):
        part = part + got[d]
    out_ref[...] = part
    settle(got, sent_sem)


def sum_squares(squares, rows):
    vmem = pl.BlockSpec(memory_space=pltpu.VMEM)
    return pl.pallas_call(
        functools.partial(norm_kernel, rows),
        out_shape=jax.ShapeDtypeStruct(squares.shape, squares.dtype),
        in_specs=[vmem],
        out_specs=vmem,
        scratch_shapes=[
            pltpu.VMEM((rows - 1,) + squares.shape, squares.dtype),
            pltpu.SemaphoreType.DMA,
            pltpu.SemaphoreType.DMA,
        ],
        compiler_params=pltpu.CompilerParams(collective_id=1, has_side_effects=True),
    )(squares)


def body(eigvecs, reflectors, factors, order, rows, cols):
    scaled = find_scaled(eigvecs, reflectors, factors, rows, cols)
    vectors, squares = update_vectors(eigvecs, reflectors, scaled)
    columns = eigvecs.shape[1]
    squares = sum_squares(jnp.sum(squares, axis=0).reshape(8, columns // 8), rows)
    return (vectors, jnp.sqrt(squares.reshape(columns) / order) - 1.0)


def solution(mesh):
    placed = (P("row", "col"), P(None, "row", None), P())
    rows, cols = mesh.shape["row"], mesh.shape["col"]

    def whole(eigvecs, reflectors, factors):
        order = eigvecs.shape[0]
        return jax.shard_map(
            lambda e, r, f: body(e, r, f, order, rows, cols),
            mesh=mesh,
            in_specs=placed,
            out_specs=(P("row", "col"), P("col")),
            check_vma=False,
        )(eigvecs, reflectors, factors)

    return whole
```

```python
import functools
import math

import jax
import jax.numpy as jnp
from jax import lax
from jax.experimental import pallas as pl
from jax.experimental.pallas import tpu as pltpu
from jax.sharding import PartitionSpec as P

MESH = pl.DeviceIdType.MESH
TN = (((0,), (0,)), ((), ()))
NT = (((1,), (1,)), ((), ()))


def settle(ref, sem):
    pltpu.make_async_copy(ref, ref, sem).wait()


def send(src, dst, sent, got, where):
    pltpu.make_async_remote_copy(
        src_ref=src, dst_ref=dst, send_sem=sent, recv_sem=got, device_id=where, device_id_type=MESH
    ).start()


def greet(axes):
    barrier = pltpu.get_barrier_semaphore()
    for axis, size in axes:
        me = lax.axis_index(axis)

        def hello(d, carry, axis=axis, size=size, me=me):
            pl.semaphore_signal(
                barrier, inc=1, device_id={axis: lax.rem(me + d, size)}, device_id_type=MESH
            )
            return carry

        lax.fori_loop(1, size, hello, 0)
    pl.semaphore_wait(barrier, sum(size - 1 for _, size in axes))


def scale_kernel(
    rows, cols, chunks,
    e_hbm, r_hbm, f_ref, out_hbm,
    ebuf, rbuf, acc, psend, xrecv, mid, precv, gsend, grecv, gbuf, xbuf, sbuf,
    e_sem, r_sem, p_sent, p_got, g_sent, g_got, h_sent, h_got, c_sent, c_got, s_sent, s_got, m_sent, m_got, x_sent, x_got, o_sem,
):
    panels, local, width = r_hbm.shape
    total = panels * width
    cw = ebuf.shape[2] // rows
    span = ebuf.shape[2]
    gs = gsend.shape[0] // rows
    depth = math.gcd(local, 1024)
    steps = local // depth
    row, col = lax.axis_index("row"), lax.axis_index("col")
    outer, half = rows // 2, span // 2
    place, side = row // 2, row % 2
    partner = {"row": row + 1 - 2 * side}
    own = pl.ds(pl.multiple_of(side * half + place * cw, cw), cw)

    def load_r(k):
        return pltpu.make_async_copy(
            r_hbm.at[k], rbuf.at[:, pl.ds(k * width, width)], r_sem.at[k]
        )

    def load_e(j):
        return pltpu.make_async_copy(
            e_hbm.at[:, pl.ds(j * span, span)], ebuf.at[j], e_sem.at[j]
        )

    for k in range(panels):
        load_r(k).start()
    for j in range(chunks):
        load_e(j).start()
    greet((("row", rows), ("col", cols)))
    for k in range(panels):
        load_r(k).wait()

    high = panels - 1 - col

    def block(t, carry):
        flag = t // high
        panel = high + flag * (col - high)
        prior = t - flag * high

        def step(i, total_block):
            at = pl.ds(pl.multiple_of(i * depth, depth), depth)
            a = rbuf[at, pl.ds(pl.multiple_of(prior * width, width), width)]
            b = rbuf[at, pl.ds(pl.multiple_of(panel * width, width), width)]
            return total_block + lax.dot_general(a, b, TN, preferred_element_type=jnp.float32)

        result = lax.fori_loop(0, steps, step, jnp.zeros((width, width), jnp.float32))
        gsend[pl.ds(pl.multiple_of(t * width, width), width), :] = result.astype(jnp.bfloat16)
        return carry

    def send_gram(d, carry):
        peer = lax.rem(row + d, rows)
        send(
            gsend.at[pl.ds(pl.multiple_of(peer * gs, gs), gs), :], grecv.at[d - 1],
            g_sent, g_got, {"row": peer},
        )
        return carry

    mine = pl.ds(pl.multiple_of(row * gs, gs), gs)

    def share_gram_rows():
        settle(grecv, g_got)
        part = gsend[mine, :].astype(jnp.float32)
        for d in range(rows - 1):
            part = part + grecv[d].astype(jnp.float32)
        gbuf[col, mine, :] = part.astype(jnp.bfloat16)

        def go(d, carry):
            peer = lax.rem(row + d, rows)
            send(gbuf.at[col, mine, :], gbuf.at[col, mine, :], h_sent, h_got, {"row": peer})
            return carry

        lax.fori_loop(1, rows, go, 0)

    def share_gram_cols():
        settle(gbuf.at[col, pl.ds(0, (rows - 1) * gs), :], h_got)

        def go(d, carry):
            peer = lax.rem(col + d, cols)
            send(gbuf.at[col], gbuf.at[col], c_sent, c_got, {"col": peer})
            return carry

        lax.fori_loop(1, cols, go, 0)

    def pass_on(j):
        settle(xrecv.at[j], p_got.at[j])
        kept = pl.ds(pl.multiple_of(side * half, half), half)
        both = psend[j, kept, :].astype(jnp.float32) + xrecv[j].astype(jnp.float32)
        mid[j] = both.astype(jnp.bfloat16)

        def go(d, carry):
            peer = lax.rem(place + d, outer)
            send(
                mid.at[j, pl.ds(pl.multiple_of(peer * cw, cw), cw), :], precv.at[j, d - 1],
                m_sent.at[j], m_got.at[j], {"row": 2 * peer + side},
            )
            return carry

        lax.fori_loop(1, outer, go, 0)

    for j in range(chunks):
        load_e(j).wait()
        acc[...] = jnp.zeros_like(acc)

        def step(i, carry, j=j):
            at = pl.ds(pl.multiple_of(i * depth, depth), depth)
            acc[...] += lax.dot_general(
                ebuf[j, at, :], rbuf[at, :], TN, preferred_element_type=jnp.float32
            )
            return carry

        lax.fori_loop(0, steps, step, 0)
        psend[j] = acc[...].astype(jnp.bfloat16)

        other = pl.ds(pl.multiple_of((1 - side) * half, half), half)
        send(psend.at[j, other, :], xrecv.at[j], p_sent.at[j], p_got.at[j], partner)
        if j == 0:
            lax.fori_loop(0, panels, block, 0)
            lax.fori_loop(1, rows, send_gram, 0)
        if j:
            pass_on(j - 1)
        if j == min(1, chunks - 1):
            share_gram_rows()
        if j == min(2, chunks - 1):
            share_gram_cols()

    pass_on(chunks - 1)
    for j in range(chunks):
        settle(precv.at[j], m_got.at[j])
        part = mid[j, pl.ds(pl.multiple_of(place * cw, cw), cw), :].astype(jnp.float32)
        for d in range(outer - 1):
            part = part + precv[j, d].astype(jnp.float32)
        xbuf[pl.ds(j * cw, cw), :] = part
    settle(gbuf.at[pl.ds(0, cols - 1)], c_got)

    done = []
    for k in range(panels):
        part = xbuf[:, k * width : (k + 1) * width]
        if k:
            slot = min(k, panels - 1 - k)
            start = 0 if k >= cols else (panels - 1 - k) * width
            cross = gbuf[slot, start : start + k * width, :]
            part = part - jnp.dot(
                jnp.concatenate(done, axis=1), cross, preferred_element_type=jnp.float32
            )
        part = lax.dot_general(
            part, f_ref[k], NT,
            precision=lax.Precision.HIGHEST, preferred_element_type=jnp.float32,
        ).astype(jnp.bfloat16)
        done.append(part)
        for j in range(chunks):
            sbuf[j, own, k * width : (k + 1) * width] = part[j * cw : (j + 1) * cw]

    send(sbuf.at[:, own, :], sbuf.at[:, own, :], x_sent, x_got, partner)

    def send_scaled(d, carry):
        peer = 2 * lax.rem(place + d, outer) + side
        send(
            sbuf.at[:, own, :], sbuf.at[:, own, :], s_sent, s_got.at[d - 1], {"row": peer}
        )
        return carry

    lax.fori_loop(1, outer, send_scaled, 0)

    def forward(d, carry):
        source = lax.rem(place + outer - d, outer)
        block = sbuf.at[:, pl.ds(pl.multiple_of(side * half + source * cw, cw), cw), :]
        settle(block, s_got.at[d - 1])
        send(block, block, x_sent, x_got, partner)
        return carry

    lax.fori_loop(1, outer, forward, 0)
    settle(grecv, g_sent)
    settle(gbuf.at[col, pl.ds(0, (rows - 1) * gs), :], h_sent)
    settle(gbuf.at[pl.ds(0, cols - 1)], c_sent)
    for j in range(chunks):
        settle(xrecv.at[j], p_sent.at[j])
        settle(precv.at[j], m_sent.at[j])
    settle(sbuf.at[:, pl.ds(0, (outer - 1) * cw), :], s_sent)
    settle(sbuf.at[:, pl.ds(0, half), :], x_got)
    settle(sbuf.at[:, pl.ds(0, half), :], x_sent)
    result = pltpu.make_async_copy(sbuf, out_hbm, o_sem)
    result.start()
    result.wait()


def find_scaled(eigvecs, reflectors, factors, rows, cols):
    local, columns = eigvecs.shape
    panels, _, width = reflectors.shape
    total = panels * width
    chunks = max(1, min(4, columns // rows // 16, columns // 128))
    span = columns // chunks
    cw = span // rows
    gs = total // rows
    any_spec = pl.BlockSpec(memory_space=pl.ANY)
    dma = pltpu.SemaphoreType.DMA
    low = jnp.bfloat16
    scaled = pl.pallas_call(
        functools.partial(scale_kernel, rows, cols, chunks),
        out_shape=jax.ShapeDtypeStruct((chunks, span, total), low),
        in_specs=[any_spec, any_spec, pl.BlockSpec(memory_space=pltpu.VMEM)],
        out_specs=any_spec,
        scratch_shapes=[
            pltpu.VMEM((chunks, local, span), low),
            pltpu.VMEM((local, total), low),
            pltpu.VMEM((span, total), jnp.float32),
            pltpu.VMEM((chunks, span, total), low),
            pltpu.VMEM((chunks, span // 2, total), low),
            pltpu.VMEM((chunks, span // 2, total), low),
            pltpu.VMEM((chunks, rows // 2 - 1, cw, total), low),
            pltpu.VMEM((total, width), low),
            pltpu.VMEM((rows - 1, gs, width), low),
            pltpu.VMEM((cols, total, width), low),
            pltpu.VMEM((chunks * cw, total), jnp.float32),
            pltpu.VMEM((chunks, span, total), low),
            dma((chunks,)), dma((panels,)), dma((chunks,)), dma((chunks,)),
            dma, dma, dma, dma, dma, dma, dma, dma((rows // 2 - 1,)),
            dma((chunks,)), dma((chunks,)), dma, dma, dma,
        ],
        compiler_params=pltpu.CompilerParams(
            collective_id=0, has_side_effects=True, vmem_limit_bytes=60 * 1024 * 1024
        ),
    )(eigvecs, reflectors, factors)
    return scaled.reshape(columns, total)


def update_kernel(e_ref, r_ref, s_ref, v_ref, q_ref):
    panels = r_ref.shape[0]
    stacked = jnp.concatenate([r_ref[k] for k in range(panels)], axis=1)
    update = lax.dot_general(stacked, s_ref[...], NT, preferred_element_type=jnp.float32)
    vectors = (e_ref[...].astype(jnp.float32) - update).astype(jnp.bfloat16)
    v_ref[...] = vectors
    wide = vectors.astype(jnp.float32)
    squares = jnp.sum((wide * wide).reshape(-1, 8, wide.shape[1]), axis=0)

    @pl.when(pl.program_id(0) == 0)
    def _():
        q_ref[...] = jnp.zeros_like(q_ref)

    q_ref[...] += squares


def update_vectors(eigvecs, reflectors, scaled):
    local, columns = eigvecs.shape
    panels, _, width = reflectors.shape
    tile = math.gcd(local, 512)
    return pl.pallas_call(
        update_kernel,
        grid=(local // tile,),
        out_shape=(
            jax.ShapeDtypeStruct((local, columns), jnp.bfloat16),
            jax.ShapeDtypeStruct((8, columns), jnp.float32),
        ),
        in_specs=[
            pl.BlockSpec((tile, columns), lambda i: (i, 0)),
            pl.BlockSpec((panels, tile, width), lambda i: (0, i, 0)),
            pl.BlockSpec((columns, panels * width), lambda i: (0, 0)),
        ],
        out_specs=(
            pl.BlockSpec((tile, columns), lambda i: (i, 0)),
            pl.BlockSpec((8, columns), lambda i: (0, 0)),
        ),
        compiler_params=pltpu.CompilerParams(
            dimension_semantics=("arbitrary",), vmem_limit_bytes=60 * 1024 * 1024
        ),
    )(eigvecs, reflectors, scaled)


def norm_kernel(rows, q_ref, out_ref, got, sent_sem, got_sem):
    row = lax.axis_index("row")
    greet((("row", rows),))

    def go(d, carry):
        send(q_ref, got.at[d - 1], sent_sem, got_sem, {"row": lax.rem(row + d, rows)})
        return carry

    lax.fori_loop(1, rows, go, 0)
    settle(got, got_sem)
    part = q_ref[...]
    for d in range(rows - 1):
        part = part + got[d]
    out_ref[...] = part
    settle(got, sent_sem)


def sum_squares(squares, rows):
    vmem = pl.BlockSpec(memory_space=pltpu.VMEM)
    return pl.pallas_call(
        functools.partial(norm_kernel, rows),
        out_shape=jax.ShapeDtypeStruct(squares.shape, squares.dtype),
        in_specs=[vmem],
        out_specs=vmem,
        scratch_shapes=[
            pltpu.VMEM((rows - 1,) + squares.shape, squares.dtype),
            pltpu.SemaphoreType.DMA,
            pltpu.SemaphoreType.DMA,
        ],
        compiler_params=pltpu.CompilerParams(collective_id=1, has_side_effects=True),
    )(squares)


def body(eigvecs, reflectors, factors, order, rows, cols):
    scaled = find_scaled(eigvecs, reflectors, factors, rows, cols)
    vectors, squares = update_vectors(eigvecs, reflectors, scaled)
    columns = eigvecs.shape[1]
    squares = sum_squares(jnp.sum(squares, axis=0).reshape(8, columns // 8), rows)
    return (vectors, jnp.sqrt(squares.reshape(columns) / order) - 1.0)


def solution(mesh):
    placed = (P("row", "col"), P(None, "row", None), P())
    rows, cols = mesh.shape["row"], mesh.shape["col"]

    def whole(eigvecs, reflectors, factors):
        order = eigvecs.shape[0]
        return jax.shard_map(
            lambda e, r, f: body(e, r, f, order, rows, cols),
            mesh=mesh,
            in_specs=placed,
            out_specs=(P("row", "col"), P("col")),
            check_vma=False,
        )(eigvecs, reflectors, factors)

    return whole
```
